128 devices in a mesh: seq: 16 (over z, y_hi, core), fsdp: 8 (over y_lo, x).
Axes of the slice: x: 4, y: 4 (y_hi: 2, y_lo: 2; y = y_hi * 2 + y_lo), z: 4, core: 2. Of those that a mesh axis runs over, the one named last changes fastest.
Arguments:
- patches: bfloat16 [8, 2048, 3072], P('fsdp', 'seq'), may hold values from -6 to 6
- weight_codes: int32 [3072, 3072], P('fsdp'), may hold values from -448 to 448
- block_scales: float32 [24, 24], P('fsdp'), may hold values from 2.5e-05 to 0.0001
- key_proj: bfloat16 [8, 2048, 3072], P('fsdp', 'seq'), may hold values from -6 to 6
- value_proj: bfloat16 [8, 2048, 3072], P('fsdp', 'seq'), may hold values from -6 to 6
- query_gain: float32 [3072], replicated, may hold values from 1 to 10
- key_gain: float32 [3072], replicated, may hold values from 1 to 10
Outputs:
- attended: bfloat16 [8, 2048, 3072], P('fsdp', 'seq')
The draws below stay inside these ranges and needn't reach their ends.
All inputs are finite; a program needn't handle non-finite values.
Results may differ from the reference program's by a relative error of at most 0.007.
The reference program's roundings to bfloat16 on the way count: a program that leaves them out, or rounds other values in their place, can miss the bound.
Values may be sent and summed in bfloat16 or wider, within the bound.
No kernel may reach another device: no remote copies, remote signals or barrier semaphores. Data moves between devices by JAX's collectives and lax.ppermute only.
A program may use at most 192 MiB of HBM per device.

```python
import math
import jax
import jax.numpy as jnp
from jax import lax

D = 3072
HEADS = 48
HDIM = 64
BLOCK = 128
IMAGES = 8
SEQ = 2048


def gain_values(key, which):
    own_key = jax.random.fold_in(key, which)
    values = jnp.exp(jax.random.uniform(own_key, (HEADS, HDIM), minval=0.0, maxval=math.log(3.0)))
    return values.reshape(HEADS * HDIM).astype(jnp.float32)


def draw_query_gain(key, part):
    return gain_values(key, 1)


def draw_key_gain(key, part):
    return gain_values(key, 2)


def touch_ends(drawn, rng, least, high):
    index_at = [jax.random.randint(jax.random.fold_in(rng, axis), (), 0, length) for axis, length in enumerate(drawn.shape)]
    longest = drawn.shape.index(max(drawn.shape))
    next_to = index_at[:longest] + [(index_at[longest] + 1) % drawn.shape[longest]] + index_at[longest + 1:]
    return drawn.at[tuple(index_at)].set(least).at[tuple(next_to)].set(high)


def block_scale(key, dims, pieces, smallest, high):
    gain, own = 1.0, jax.random.fold_in(key, 6)
    for dim, shards_of in pieces:
        steps = jnp.exp(jax.random.uniform(jax.random.fold_in(own, dim), (shards_of,), jnp.float32, smallest / len(pieces), high / len(pieces)))
        gain = gain * jnp.repeat(steps, dims[dim] // shards_of).reshape([-1 if axis == dim else 1 for axis in range(len(dims))])
    return gain


def bell_draw(key, shape, deviation, limit, shards=(), held_as=jnp.bfloat16):
    values = deviation * jax.random.normal(key, shape, jnp.float32)
    if shards:
        values = values * block_scale(key, shape, shards, -0.22, 0.18)
    return jnp.clip(values, -limit, limit).astype(held_as)


def setup_inputs(seed: int = 0) -> dict:
    keys = jax.random.split(jax.random.key(seed), 8)
    return {
        "patches": bell_draw(keys[0], (IMAGES, SEQ, D), 1.0, 6.0, ((0, 8), (1, 16))),
        "weight_codes": touch_ends(jax.random.randint(keys[1], (D, HEADS * HDIM), -448, 449), jax.random.fold_in(keys[1], 1), -448, 448).astype(jnp.int32),
        "block_scales": jnp.clip(jnp.exp(math.log(0.0001) - 1.3862944 * jax.random.uniform(keys[2], (D // BLOCK, HEADS * HDIM // BLOCK), jnp.float32) ** block_scale(keys[2], (D // BLOCK, HEADS * HDIM // BLOCK), ((0, 8),), -0.2, 0.2)), 2.499999936844688e-05, 0.0001),
        "key_proj": bell_draw(keys[3], (IMAGES, SEQ, HEADS * HDIM), 1.0, 6.0, ((0, 8), (1, 16))),
        "value_proj": bell_draw(keys[4], (IMAGES, SEQ, HEADS * HDIM), 1.0, 6.0, ((0, 8), (1, 16))),
        "query_gain": draw_query_gain(jax.random.fold_in(keys[7], 71), 0),
        "key_gain": draw_key_gain(jax.random.fold_in(keys[7], 71), 0),
    }


NORM_FLOOR = 0.25

def head_norm(projected, gain_row):
    shaped = projected.reshape(projected.shape[:-1] + (HEADS, HDIM))
    average = lax.optimization_barrier(jnp.mean(shaped, axis=-1, keepdims=True))
    centred = shaped - average
    spread = lax.optimization_barrier(jnp.mean(centred * centred, axis=-1, keepdims=True))
    normed = centred * lax.rsqrt(spread + NORM_FLOOR) * gain_row.reshape(HEADS, HDIM)
    return normed.astype(jnp.bfloat16)

def reference(patches, weight_codes, block_scales, key_proj, value_proj, query_gain, key_gain):
    column_count = HEADS * HDIM
    blocked = weight_codes.astype(jnp.float32).reshape(D // BLOCK, BLOCK, column_count // BLOCK, BLOCK)
    weight = (blocked * block_scales[:, None, :, None]).reshape(D, column_count).astype(jnp.bfloat16)
    queries = jnp.dot(patches.reshape(IMAGES * SEQ, D), weight, preferred_element_type=jnp.float32)
    queries = queries.reshape(IMAGES, SEQ, column_count)
    query_view = head_norm(queries, query_gain)
    key_view = head_norm(key_proj.astype(jnp.float32), key_gain)
    value_view = value_proj.reshape(IMAGES, SEQ, HEADS, HDIM)

    def one_head(members):
        query_head, key_head, value_head = members
        scores = jnp.einsum('iqd,ikd->iqk', query_head.astype(jnp.float32), key_head.astype(jnp.float32)) * HDIM ** (-0.5)
        largest = lax.optimization_barrier(jnp.max(scores, axis=-1, keepdims=True))
        probability = jnp.exp(scores - largest)
        normaliser = lax.optimization_barrier(jnp.sum(probability, axis=-1))
        rounded = lax.optimization_barrier(probability.astype(jnp.bfloat16))
        blended = jnp.einsum('iqk,ikd->iqd', rounded.astype(jnp.float32), value_head.astype(jnp.float32))
        return blended / normaliser[..., None]
    outputs = lax.map(one_head, (jnp.moveaxis(query_view, 2, 0), jnp.moveaxis(key_view, 2, 0), jnp.moveaxis(value_view, 2, 0)))
    return jnp.moveaxis(outputs, 0, 2).reshape(IMAGES, SEQ, column_count).astype(jnp.bfloat16)
```

```python
import math

import jax
import jax.numpy as jnp
from jax import lax
from jax.experimental import pallas as pl
from jax.experimental.pallas import tpu as pltpu
from jax.sharding import Mesh
from jax.sharding import PartitionSpec as P

HEADS = 48
HDIM = 64
BLOCK = 128
NORM_FLOOR = 0.25
EXP2_SCALE = HDIM**-0.5 * math.log2(math.e)
QUERY_BLOCK = 256
KEY_CHUNK = 128
LANES = 128
COLUMN_BLOCK = 256
SEQ = ("z", "yh", "co")
FSDP = ("yl", "x")
Z, X = 4, 4


def head_norm(projected, gain_row):
    shaped = projected.reshape(projected.shape[:-1] + (-1, HDIM))
    average = jnp.mean(shaped, axis=-1, keepdims=True)
    centred = shaped - average
    spread = jnp.mean(centred * centred, axis=-1, keepdims=True)
    normed = centred * lax.rsqrt(spread + NORM_FLOOR) * gain_row.reshape(-1, HDIM)
    return normed.astype(jnp.bfloat16).reshape(projected.shape)


def dequantize(weight_codes, block_scales):
    row_count, column_count = weight_codes.shape
    blocked = weight_codes.astype(jnp.float32).reshape(
        row_count // BLOCK, BLOCK, column_count // BLOCK, BLOCK
    )
    return (
        (blocked * block_scales[:, None, :, None])
        .reshape(row_count, column_count)
        .astype(jnp.bfloat16)
    )


def shift(value, axis, by, size):
    return lax.ppermute(value, axis, [(i, (i + by) % size) for i in range(size)])


def project_and_attend(tokens, weights, pairs, gain):
    token_counts = [t.shape[0] for t in tokens]
    key_counts = [p.shape[1] for p in pairs]
    total, keys = sum(token_counts), sum(key_counts)
    features, columns = tokens[0].shape[1], weights[0].shape[1]
    heads = COLUMN_BLOCK // HDIM
    blocks = total // QUERY_BLOCK
    units = heads * blocks
    nt, nw, nk = len(tokens), len(weights), len(pairs)

    def body(*refs):
        token_refs, refs = refs[:nt], refs[nt:]
        weight_refs, refs = refs[:nw], refs[nw:]
        key_refs, refs = refs[:nk], refs[nk:]
        value_refs, refs = refs[:nk], refs[nk:]
        gain_ref, refs = refs[0], refs[1:]
        out_refs, refs = refs[:nt], refs[nt:]
        query_ref, value_t, score_ref, prob_ref, out_t, max_ref = refs

        at = 0
        for t, token_ref in enumerate(token_refs):
            count = token_counts[t]
            acc, row = None, 0
            for weight_ref in weight_refs:
                rows = weight_ref.shape[0]
                part = jnp.dot(
                    token_ref[:, row : row + rows],
                    weight_ref[...],
                    preferred_element_type=jnp.float32,
                )
                acc = part if acc is None else acc + part
                row += rows
            turned = acc.T.reshape(heads, HDIM, count)
            centred = turned - jnp.mean(turned, axis=1, keepdims=True)
            spread = jnp.mean(centred * centred, axis=1, keepdims=True)
            gains = gain_ref[...].reshape(heads, HDIM, 1)
            normed = (centred * lax.rsqrt(spread + NORM_FLOOR) * gains).astype(jnp.bfloat16)
            nothing = jnp.zeros((HDIM, count), jnp.bfloat16)
            for h in range(heads):
                low, high = (normed[h], nothing) if h % 2 == 0 else (nothing, normed[h])
                query_ref[h, 0:HDIM, at : at + count] = low
                query_ref[h, HDIM : 2 * HDIM, at : at + count] = high
            at += count
        at = 0
        for value_ref in value_refs:
            count = value_ref.shape[0]
            value_t[:, at : at + count] = value_ref[...].T
            at += count

        def scores(unit, slot):
            h, b = unit // blocks, unit % blocks
            query = query_ref[h, :, pl.ds(pl.multiple_of(b * QUERY_BLOCK, QUERY_BLOCK), QUERY_BLOCK)]
            lanes = pl.ds(pl.multiple_of((h // 2) * LANES, LANES), LANES)
            at, top = 0, None
            for key_ref in key_refs:
                for c in range(key_ref.shape[0] // KEY_CHUNK):
                    score = jnp.dot(
                        key_ref[c * KEY_CHUNK : (c + 1) * KEY_CHUNK, lanes],
                        query,
                        preferred_element_type=jnp.float32,
                    )
                    score_ref[slot, at : at + KEY_CHUNK, :] = score
                    best = jnp.max(score.reshape(KEY_CHUNK // 8, 8, QUERY_BLOCK), axis=0)
                    top = best if top is None else jnp.maximum(top, best)
                    at += KEY_CHUNK
            max_ref[slot] = top

        def finish(unit, slot):
            h, b = unit // blocks, unit % blocks
            top = jnp.max(max_ref[slot], axis=0, keepdims=True)
            total_sum = None
            for c in range(keys // KEY_CHUNK):
                at = c * KEY_CHUNK
                prob = jnp.exp2((score_ref[slot, at : at + KEY_CHUNK, :] - top) * EXP2_SCALE)
                part = jnp.sum(prob.reshape(KEY_CHUNK // 8, 8, QUERY_BLOCK), axis=0)
                total_sum = part if total_sum is None else total_sum + part
                prob_ref[at : at + KEY_CHUNK, :] = prob.astype(jnp.bfloat16)
            rows = pl.ds(pl.multiple_of(h * HDIM, HDIM), HDIM)
            blended = jnp.dot(value_t[rows, :], prob_ref[...], preferred_element_type=jnp.float32)
            norm = jnp.sum(total_sum, axis=0, keepdims=True)
            out_t[rows, pl.ds(pl.multiple_of(b * QUERY_BLOCK, QUERY_BLOCK), QUERY_BLOCK)] = (
                blended / norm
            )

        scores(0, 0)

        def step(unit, carry):
            slot = unit % 2
            scores(jnp.minimum(unit + 1, units - 1), 1 - slot)
            finish(unit, slot)
            return carry

        lax.fori_loop(0, units, step, 0)
        at = 0
        for t, out_ref in enumerate(out_refs):
            out_ref[...] = out_t[:, at : at + token_counts[t]].T.astype(jnp.bfloat16)
            at += token_counts[t]

    def half(count, which):
        return pl.BlockSpec((None, count, COLUMN_BLOCK), lambda i: (which, 0, i))

    return pl.pallas_call(
        body,
        grid=(columns // COLUMN_BLOCK,),
        in_specs=[pl.BlockSpec((t, features), lambda i: (0, 0)) for t in token_counts]
        + [pl.BlockSpec((w.shape[0], COLUMN_BLOCK), lambda i: (0, i)) for w in weights]
        + [half(n, 0) for n in key_counts]
        + [half(n, 1) for n in key_counts]
        + [pl.BlockSpec((COLUMN_BLOCK, 1), lambda i: (i, 0))],
        out_specs=[pl.BlockSpec((t, COLUMN_BLOCK), lambda i: (0, i)) for t in token_counts],
        out_shape=[jax.ShapeDtypeStruct((t, columns), jnp.bfloat16) for t in token_counts],
        scratch_shapes=[
            pltpu.VMEM((heads, 2 * HDIM, total), jnp.bfloat16),
            pltpu.VMEM((COLUMN_BLOCK, keys), jnp.bfloat16),
            pltpu.VMEM((2, keys, QUERY_BLOCK), jnp.float32),
            pltpu.VMEM((keys, QUERY_BLOCK), jnp.bfloat16),
            pltpu.VMEM((COLUMN_BLOCK, total), jnp.float32),
            pltpu.VMEM((2, 8, QUERY_BLOCK), jnp.float32),
        ],
        compiler_params=pltpu.CompilerParams(
            dimension_semantics=("arbitrary",), vmem_limit_bytes=56 << 20
        ),
    )(*tokens, *weights, *pairs, *pairs, gain)


def per_device(patches, weight_codes, block_scales, key_proj, value_proj, query_gain, key_gain):
    tokens, features = patches.shape[1:]
    rows = weight_codes.shape[0]
    share = features // Z
    z, co, yl, x = (lax.axis_index(a) for a in ("z", "co", "yl", "x"))

    both = jnp.stack([head_norm(key_proj[0].astype(jnp.float32), key_gain), value_proj[0]])

    def quarter(by):
        at = ((z + by) % Z) * share
        return lax.dynamic_slice(both, (0, 0, at), (2, tokens, share))

    near = quarter(0)
    far = jnp.concatenate([shift(quarter(by), "z", by, Z) for by in (1, 3, 2)], axis=1)
    pairs = [near, far, shift(near, "yh", 1, 2), shift(far, "yh", 1, 2)]
    pairs = pairs + [shift(p, "co", 1, 2) for p in pairs]

    own = dequantize(
        lax.dynamic_slice(weight_codes, (0, z * share), (rows, share)),
        lax.dynamic_slice(
            block_scales, (0, z * (share // BLOCK)), (rows // BLOCK, share // BLOCK)
        ),
    )
    y_moves = []
    for y in range(4):
        for core, by in ((0, 1), (1, 3)):
            to = (y + by) % 4
            y_moves.append((((y // 2) * 2 + core) * 2 + y % 2, ((to // 2) * 2 + core) * 2 + to % 2))
    half = rows // 2
    mine = lax.ppermute(
        lax.dynamic_slice(own, (co * half, 0), (half, share)), ("yh", "co", "yl"), y_moves
    )
    theirs = shift(mine, "co", 1, 2)
    unit = jnp.concatenate(
        [own, jnp.where(co == 0, mine, theirs), jnp.where(co == 0, theirs, mine)]
    )
    x_moves = [(core * X + i, core * X + (i + by) % X) for core, by in ((0, 1), (1, 3)) for i in range(X)]
    mine_near = lax.ppermute(unit, ("co", "x"), x_moves)
    mine_far = shift(lax.dynamic_slice(unit, (co * rows, 0), (rows, share)), "x", 2, X)
    weights = [unit, mine_near, mine_far, shift(mine_near, "co", 1, 2), shift(mine_far, "co", 1, 2)]

    back = jnp.where(co == 0, 3, 1)
    order = [
        (yl, x),
        (1 - yl, x),
        (yl, x + back),
        (1 - yl, x + back),
        ((yl + co) % 2, x + 2),
        (yl, x + 4 - back),
        (1 - yl, x + 4 - back),
        ((yl + 1 - co) % 2, x + 2),
    ]
    ordered = jnp.concatenate(
        [
            lax.dynamic_slice(patches[0], (0, (a * X + b % X) * rows), (tokens, rows))
            for a, b in order
        ],
        axis=1,
    )
    steps = (0, 1, 3, 2)
    arrived = [ordered] + [shift(ordered, "z", by, Z) for by in steps[1:]]

    gain = lax.dynamic_slice(query_gain, (z * share,), (share,)).reshape(share, 1)
    done = project_and_attend(arrived, weights, pairs, gain)
    result = jnp.zeros((tokens, features), jnp.bfloat16)
    for by, piece in zip(steps, done):
        if by:
            piece = shift(piece, "z", Z - by, Z)
        result = lax.dynamic_update_slice(result, piece, (0, ((z + by) % Z) * share))
    return result[None]


def solution(mesh):
    split = Mesh(mesh.devices.reshape(Z, 2, 2, 2, X), ("z", "yh", "co", "yl", "x"))
    placed = (
        P(FSDP, SEQ, None),
        P(FSDP, None),
        P(FSDP, None),
        P(FSDP, SEQ, None),
        P(FSDP, SEQ, None),
        P(),
        P(),
    )
    return jax.shard_map(
        per_device, mesh=split, in_specs=placed, out_specs=P(FSDP, SEQ, None), check_vma=False
    )
```

```python
import math

import jax
import jax.numpy as jnp
from jax import lax
from jax.experimental import pallas as pl
from jax.experimental.pallas import tpu as pltpu
from jax.sharding import Mesh
from jax.sharding import PartitionSpec as P

HDIM = 64
BLOCK = 128
NORM_FLOOR = 0.25
EXP2_SCALE = HDIM**-0.5 * math.log2(math.e)
ROW_BLOCK = 384
KEY_CHUNK = 256
GROUPS = ((0, 1, 2), (3, 4, 5), (6, 7, 8), (9, 10, 11))
LANES = 128
COLUMN_BLOCK = 256
SEQ = ("z", "yh", "co")
FSDP = ("yl", "x")
Z, X = 4, 4


def dequantize(weight_codes, block_scales):
    row_count, column_count = weight_codes.shape
    blocked = weight_codes.astype(jnp.float32).reshape(
        row_count // BLOCK, BLOCK, column_count // BLOCK, BLOCK
    )
    return (
        (blocked * block_scales[:, None, :, None])
        .reshape(row_count, column_count)
        .astype(jnp.bfloat16)
    )


def shift(value, axis, by, size):
    return lax.ppermute(value, axis, [(i, (i + by) % size) for i in range(size)])


def prepare(position, keys, values, gain, steps):
    count, features = keys.shape
    share = features // Z

    def body(position_ref, key_ref, value_ref, gain_ref, *out_refs):
        for by, out_ref in zip(steps, out_refs):
            at = pl.ds(pl.multiple_of(((position_ref[0] + by) % Z) * share, LANES), share)
            turned = key_ref[:, at].astype(jnp.float32).T.reshape(share // HDIM, HDIM, count)
            centred = turned - jnp.mean(turned, axis=1, keepdims=True)
            spread = jnp.mean(centred * centred, axis=1, keepdims=True)
            normed = (centred * lax.rsqrt(spread + NORM_FLOOR)).reshape(share, count)
            out_ref[0] = (normed.T * gain_ref[:, at]).astype(jnp.bfloat16)
            out_ref[1] = value_ref[:, at]

    whole = pl.BlockSpec(memory_space=pltpu.VMEM)
    return pl.pallas_call(
        body,
        in_specs=[pl.BlockSpec(memory_space=pltpu.SMEM), whole, whole, whole],
        out_specs=[whole for _ in steps],
        out_shape=[pltpu.VMEM((2, count, share), jnp.bfloat16) for _ in steps],
    )(position, keys, values, gain.reshape(1, features))


def assemble(position, pieces, steps):
    count, share = pieces[0].shape

    def body(position_ref, *refs):
        out_ref = refs[-1]
        for by, ref in zip(steps, refs[:-1]):
            at = pl.ds(pl.multiple_of(((position_ref[0] + by) % Z) * share, LANES), share)
            out_ref[0, :, at] = ref[...]

    whole = pl.BlockSpec(memory_space=pltpu.VMEM)
    return pl.pallas_call(
        body,
        in_specs=[pl.BlockSpec(memory_space=pltpu.SMEM)] + [whole for _ in pieces],
        out_specs=whole,
        out_shape=jax.ShapeDtypeStruct((1, count, share * Z), jnp.bfloat16),
    )(position, *[in_vmem(p) for p in pieces])


def project_and_attend(order, tokens, weights, pairs, gain):
    token_counts = [t.shape[0] for t in tokens]
    key_counts = [p.shape[1] for p in pairs]
    total, keys = sum(token_counts), sum(key_counts)
    features, columns = tokens[0].shape[1], weights[0].shape[1]
    heads, block_heads = columns // HDIM, COLUMN_BLOCK // HDIM
    nt, nw, nk = len(tokens), len(weights), len(pairs)

    def body(order_ref, *refs):
        token_refs, refs = refs[:nt], refs[nt:]
        weight_refs, refs = refs[:nw], refs[nw:]
        pair_refs, refs = refs[:nk], refs[nk:]
        gain_ref, refs = refs[0], refs[1:]
        out_refs, refs = refs[:nt], refs[nt:]
        sorted_ref, query_ref, value_t, score_a, score_b, top_a, top_b, out_t = refs
        for j in range(features // ROW_BLOCK):
            src = pl.ds(pl.multiple_of(order_ref[j] * ROW_BLOCK, LANES), ROW_BLOCK)
            at = 0
            for t, ref in enumerate(token_refs):
                sorted_ref[at : at + token_counts[t], j * ROW_BLOCK : (j + 1) * ROW_BLOCK] = ref[:, src]
                at += token_counts[t]

        def project(i, carry):
            cols = pl.ds(pl.multiple_of(i * COLUMN_BLOCK, COLUMN_BLOCK), COLUMN_BLOCK)
            queries = jnp.dot(
                sorted_ref[...],
                jnp.concatenate([w[:, cols] for w in weight_refs], axis=0),
                preferred_element_type=jnp.float32,
            )
            turned = queries.T.reshape(block_heads, HDIM, total)
            centred = turned - jnp.mean(turned, axis=1, keepdims=True)
            spread = jnp.mean(centred * centred, axis=1, keepdims=True)
            gains = gain_ref[cols, :].reshape(block_heads, HDIM, 1)
            normed = (centred * lax.rsqrt(spread + NORM_FLOOR) * gains).astype(jnp.bfloat16)
            scaled = normed.astype(jnp.float32) * EXP2_SCALE
            high = scaled.astype(jnp.bfloat16)
            low = (scaled - high.astype(jnp.float32)).astype(jnp.bfloat16)
            nothing = jnp.zeros((HDIM, total), jnp.bfloat16)
            for h in range(block_heads):
                at = i * block_heads + h
                for part, value in enumerate((high[h], low[h])):
                    up, down = (value, nothing) if h % 2 == 0 else (nothing, value)
                    query_ref[at, part * LANES : part * LANES + HDIM] = up
                    query_ref[at, part * LANES + HDIM : (part + 1) * LANES] = down
            at = 0
            for ref in pair_refs:
                n = ref.shape[1]
                value_t[cols, at : at + n] = ref[1, :, cols].T
                at += n
            return carry

        lax.fori_loop(0, columns // COLUMN_BLOCK, project, 0)

        def scores(h, score_ref, top_ref):
            lanes = pl.ds(pl.multiple_of((h // 2) * LANES, LANES), LANES)
            at, top = 0, None
            for group in GROUPS:
                key = jnp.concatenate([pair_refs[g][0, :, lanes] for g in group], axis=0)
                n = key.shape[0]
                score = jnp.dot(
                    jnp.concatenate([key, key], axis=1),
                    query_ref[h],
                    preferred_element_type=jnp.float32,
                )
                score_ref[at : at + n] = score
                best = jnp.max(score.reshape(n // 8, 8, total), axis=0)
                top = best if top is None else jnp.maximum(top, best)
                at += n
            top_ref[...] = top

        def finish(h, score_ref, top_ref):
            rows = pl.ds(pl.multiple_of(h * HDIM, HDIM), HDIM)
            top = jnp.max(top_ref[...], axis=0, keepdims=True)
            sums, blend = None, None
            for at in range(0, keys, KEY_CHUNK):
                prob = jnp.exp2(score_ref[at : at + KEY_CHUNK] - top)
                part = jnp.sum(prob.reshape(KEY_CHUNK // 8, 8, total), axis=0)
                sums = part if sums is None else sums + part
                more = jnp.dot(
                    value_t[rows, at : at + KEY_CHUNK],
                    prob.astype(jnp.bfloat16),
                    preferred_element_type=jnp.float32,
                )
                blend = more if blend is None else blend + more
            out_t[rows] = blend / jnp.sum(sums, axis=0, keepdims=True)

        scores(0, score_a, top_a)

        def pair(p, carry):
            @pl.when(p >= 0)
            def _():
                finish(2 * p, score_a, top_a)
                scores(2 * p + 1, score_b, top_b)

            @pl.when(p < heads)
            def _():
                finish(2 * p + 1, score_b, top_b)
                scores(jnp.minimum(2 * p + 2, heads - 1), score_a, top_a)

            return carry

        lax.fori_loop(0, heads // 2, pair, 0)
        at = 0
        for t, ref in enumerate(out_refs):
            ref[...] = out_t[:, at : at + token_counts[t]].T.astype(jnp.bfloat16)
            at += token_counts[t]

    inside = pl.BlockSpec(memory_space=pltpu.VMEM)
    operands = [in_vmem(v) for v in (*tokens, *weights, *pairs, gain)]
    return pl.pallas_call(
        body,
        in_specs=[pl.BlockSpec(memory_space=pltpu.SMEM)] + [inside] * len(operands),
        out_specs=[inside] * nt,
        scratch_shapes=[
            pltpu.VMEM((total, features), jnp.bfloat16),
            pltpu.VMEM((heads, 2 * LANES, total), jnp.bfloat16),
            pltpu.VMEM((columns, keys), jnp.bfloat16),
            pltpu.VMEM((keys, total), jnp.float32),
            pltpu.VMEM((keys, total), jnp.float32),
            pltpu.VMEM((8, total), jnp.float32),
            pltpu.VMEM((8, total), jnp.float32),
            pltpu.VMEM((columns, total), jnp.float32),
        ],
        out_shape=[pltpu.VMEM((t, columns), jnp.bfloat16) for t in token_counts],
        compiler_params=pltpu.CompilerParams(vmem_limit_bytes=24 << 20),
    )(order, *operands)


def in_vmem(value):
    return pltpu.with_memory_space_constraint(value, pltpu.VMEM)


def layer(patches, weight_codes, block_scales, key_proj, value_proj, query_gain, key_gain):
    _, features = patches.shape[1:]
    rows = weight_codes.shape[0]
    share = features // Z
    z, co, yl, x = (lax.axis_index(a) for a in ("z", "co", "yl", "x"))
    position = z.astype(jnp.int32).reshape(1)
    steps = (0, 1, 3, 2)

    own = dequantize(
        lax.dynamic_slice(weight_codes, (0, z * share), (rows, share)),
        lax.dynamic_slice(
            block_scales, (0, z * (share // BLOCK)), (rows // BLOCK, share // BLOCK)
        ),
    )
    y_moves = []
    for y in range(4):
        for core, by in ((0, 1), (1, 3)):
            to = (y + by) % 4
            y_moves.append((((y // 2) * 2 + core) * 2 + y % 2, ((to // 2) * 2 + core) * 2 + to % 2))
    x_moves = [
        (core * X + i, core * X + (i + by) % X) for core, by in ((0, 1), (1, 3)) for i in range(X)
    ]
    other = lax.ppermute(own, ("yh", "co", "yl"), y_moves)
    near_own = lax.ppermute(own, ("co", "x"), x_moves)
    near_other = lax.ppermute(other, ("co", "x"), x_moves)
    mine_far = shift(jnp.where(co == 0, own, other), "x", 2, X)
    weights = [
        own,
        other,
        near_own,
        near_other,
        mine_far,
        shift(near_own, "co", 1, 2),
        shift(near_other, "co", 1, 2),
        shift(mine_far, "co", 1, 2),
    ]

    near, first, third, second = prepare(position, key_proj[0], value_proj[0], key_gain, steps)
    sent = [shift(piece, "z", by, Z) for by, piece in ((1, first), (3, third), (2, second))]
    near_y = shift(near, "yh", 1, 2)
    middle = jnp.concatenate(sent[:2], axis=1)
    middle_y = shift(middle, "yh", 1, 2)
    far = sent[2]
    far_y = shift(far, "yh", 1, 2)
    pieces = {
        "near": near,
        "middle": middle,
        "far": far,
        "neary": near_y,
        "middley": middle_y,
        "fary": far_y,
    }
    pairs = list(pieces.values())
    pairs += [shift(piece, "co", 1, 2) for piece in pieces.values()]

    back = jnp.where(co == 0, 3, 1)
    order = jnp.stack(
        [
            a * X + b % X
            for a, b in (
                (yl, x),
                (1 - yl, x),
                (yl, x + back),
                (1 - yl, x + back),
                ((yl + co) % 2, x + 2),
                (yl, x + 4 - back),
                (1 - yl, x + 4 - back),
                ((yl + 1 - co) % 2, x + 2),
            )
        ]
    ).astype(jnp.int32)
    arrived = {by: shift(patches[0], "z", by, Z) for by in (1, 3, 2)}
    gain = lax.dynamic_slice(query_gain, (z * share,), (share,)).reshape(share, 1)
    done = {}
    done[1], done[3] = project_and_attend(order, [arrived[1], arrived[3]], weights, pairs, gain)
    done[2], done[0] = project_and_attend(order, [arrived[2], patches[0]], weights, pairs, gain)
    pieces = [shift(done[by], "z", Z - by, Z) if by else done[by] for by in steps]
    return assemble(position, pieces, steps)


def solution(mesh):
    split = Mesh(mesh.devices.reshape(Z, 2, 2, 2, X), ("z", "yh", "co", "yl", "x"))
    placed = (
        P(FSDP, SEQ, None),
        P(FSDP, None),
        P(FSDP, None),
        P(FSDP, SEQ, None),
        P(FSDP, SEQ, None),
        P(),
        P(),
    )
    return jax.shard_map(
        layer, mesh=split, in_specs=placed, out_specs=P(FSDP, SEQ, None), check_vma=False
    )
```
